32 devices in a mesh: gx: 4 (over y, x), gy: 4 (over z), gz: 2 (over core).
Axes of the slice: x: 2, y: 2, z: 4, core: 2. Of those that a mesh axis runs over, the one named last changes fastest.
Arguments:
- positions: float32 [12, 12, 16, 96], P('gx', 'gy', 'gz'), may hold values from 0 to 1
- types: int32 [12, 12, 16, 32], P('gx', 'gy', 'gz'), may hold values from 0 to 2
Outputs:
- forces_energy: float32 [12, 12, 16, 128], P('gx', 'gy', 'gz')
The draws below stay inside these ranges and needn't reach their ends.
Inputs may be any that keep to these rules, and one draw needn't show every extreme that they name: `types`: 0 marks an empty slot, 1 a copper atom, 2 a nickel atom.
All inputs are finite; a program needn't handle non-finite values.
Results may differ from the reference program's by a relative error of at most 0.0001.
Values sent between devices are 32-bit elements; how exact they have to be, the bound alone decides.
A program may use at most 64 MiB of HBM per device.

```python
import jax
import jax.numpy as jnp
from jax import lax

S = 32
NX = 12
NY = 12
NZ = 16


def set_ends(entries, key, least, top_value):
    index_at = [jax.random.randint(jax.random.fold_in(key, axis), (), 0, length) for axis, length in enumerate(entries.shape)]
    main_axis = entries.shape.index(max(entries.shape))
    beside = index_at[:main_axis] + [(index_at[main_axis] + 1) % entries.shape[main_axis]] + index_at[main_axis + 1:]
    return entries.at[tuple(index_at)].set(least).at[tuple(beside)].set(top_value)


def shard_levels(stream_key, dims, cuts, smallest, largest):
    level, own = 1.0, jax.random.fold_in(stream_key, 6)
    for axis_at, shards_of in cuts:
        draws = jnp.exp(jax.random.uniform(jax.random.fold_in(own, axis_at), (shards_of,), jnp.float32, smallest / len(cuts), largest / len(cuts)))
        level = level * jnp.repeat(draws, dims[axis_at] // shards_of).reshape([-1 if axis == axis_at else 1 for axis in range(len(dims))])
    return level


def setup_inputs(seed: int = 0) -> dict:
    key_list = jax.random.split(jax.random.key(seed), 3)
    return {
        "positions": jnp.clip(1.0 * jax.random.uniform(key_list[0], (NX, NY, NZ, 3 * S), jnp.float32) ** shard_levels(key_list[0], (NX, NY, NZ, 3 * S), ((0, 4), (1, 4), (2, 2)), -0.2, 0.2), 0.0, 1.0),
        "types": set_ends(jax.random.randint(key_list[1], (NX, NY, NZ, S), 0, 3), jax.random.fold_in(key_list[1], 1), 0, 2).astype(jnp.int32),
    }


cut_square = 0.9025
density_rate = 3.0
pair_rate = 6.0

def type_tables(types):
    weight = jnp.where(types == 1, 1.0, jnp.where(types == 2, 1.6, 0.0)).astype(jnp.float32)
    embedding = jnp.where(types == 1, 1.0, jnp.where(types == 2, 1.4, 0.0)).astype(jnp.float32)
    return (weight, embedding)

def separation(own_coords, other_coords, cell_shift):
    shift_vector = jnp.asarray(cell_shift, jnp.float32).reshape(3, 1, 1)
    displace = shift_vector + other_coords[..., :, None, :] - own_coords[..., :, :, None]
    return (displace, lax.optimization_barrier(jnp.sum(displace * displace, axis=-3)))

def density_shape(square):
    margin = jnp.maximum(1.0 - square / cut_square, 0.0)
    return jnp.exp(-density_rate * square) * margin * margin

def all_shapes(square):
    margin = jnp.maximum(1.0 - square / cut_square, 0.0)
    density_exponent = jnp.exp(-density_rate * square)
    pair_exp = jnp.exp(-pair_rate * square)
    dens_slope = -density_exponent * margin * (density_rate * margin + 2.0 / cut_square)
    pair_value = pair_exp * margin * margin
    pair_slope = -pair_exp * margin * (pair_rate * margin + 2.0 / cut_square)
    return (dens_slope, pair_value, pair_slope)

def neighbour_shifts():
    return [(a, b, c) for a in (-1, 0, 1) for b in (-1, 0, 1) for c in (-1, 0, 1)]

def reference(positions, types):
    size_x, size_y, size_z, slots = types.shape
    coords = positions.reshape(size_x, size_y, size_z, 3, slots)
    weight, embedding = type_tables(types)
    margins = ((1, 1), (1, 1), (1, 1), (0, 0))
    pad_coords = jnp.pad(coords, margins + ((0, 0),), mode='wrap')
    pad_weight = jnp.pad(weight, margins, mode='wrap')
    distinct = 1.0 - jnp.eye(slots, dtype=jnp.float32)
    plane_ids = jnp.arange(size_x).astype(jnp.int32)

    def neighbour(padded, plane_index, cell_shift):
        x_layer = lax.dynamic_index_in_dim(padded, plane_index + 1 + cell_shift[0], 0, keepdims=False)
        return x_layer[1 + cell_shift[1]:1 + cell_shift[1] + size_y, 1 + cell_shift[2]:1 + cell_shift[2] + size_z]

    def own_plane(array, plane_index):
        return lax.dynamic_index_in_dim(array, plane_index, 0, keepdims=False)

    def density_plane(plane_index):
        own_coords = own_plane(coords, plane_index)
        summed = jnp.zeros((size_y, size_z, slots), jnp.float32)
        for cell_shift in neighbour_shifts():
            other_coords = neighbour(pad_coords, plane_index, cell_shift)
            other_weight = neighbour(pad_weight, plane_index, cell_shift)
            displace, square = separation(own_coords, other_coords, cell_shift)
            dens = density_shape(square)
            if cell_shift == (0, 0, 0):
                dens = dens * distinct
            summed = summed + lax.optimization_barrier(jnp.sum(dens * other_weight[..., None, :], axis=-1))
        return summed
    density_sum = lax.map(density_plane, plane_ids)
    root_value = jnp.sqrt(density_sum + 1.0)
    slope = -embedding / (2.0 * root_value)
    pad_slope = jnp.pad(slope, margins, mode='wrap')

    def force_plane(plane_index):
        own_coords = own_plane(coords, plane_index)
        own_weight = own_plane(weight, plane_index)
        own_slope = own_plane(slope, plane_index)
        force_sum = jnp.zeros((size_y, size_z, 3, slots), jnp.float32)
        pair_sum = jnp.zeros((size_y, size_z, slots), jnp.float32)
        for cell_shift in neighbour_shifts():
            other_coords = neighbour(pad_coords, plane_index, cell_shift)
            other_weight = neighbour(pad_weight, plane_index, cell_shift)
            other_slope = neighbour(pad_slope, plane_index, cell_shift)
            displace, square = separation(own_coords, other_coords, cell_shift)
            dens_slope, pair_value, pair_slope = all_shapes(square)
            both_weight = own_weight[..., :, None] * other_weight[..., None, :]
            coupling = (own_slope[..., :, None] * other_weight[..., None, :] + other_slope[..., None, :] * own_weight[..., :, None]) * dens_slope + 0.5 * both_weight * pair_slope
            energy_pair = 0.25 * both_weight * pair_value
            if cell_shift == (0, 0, 0):
                coupling = coupling * distinct
                energy_pair = energy_pair * distinct
            force_sum = force_sum + 2.0 * lax.optimization_barrier(jnp.sum(coupling[..., None, :, :] * displace, axis=-1))
            pair_sum = pair_sum + lax.optimization_barrier(jnp.sum(energy_pair, axis=-1))
        return (force_sum, pair_sum)
    force_all, pair_all = lax.map(force_plane, plane_ids)
    energy_all = pair_all - embedding * root_value
    return jnp.concatenate([force_all.reshape(size_x, size_y, size_z, 3 * slots), energy_all], axis=-1)
```

```python
import functools
import math

import jax
import jax.numpy as jnp
from jax import lax
from jax.experimental import pallas as pl
from jax.experimental.pallas import tpu as pltpu
from jax.sharding import PartitionSpec as P

cut_square = 0.9025
density_rate = 3.0
unit = density_rate * math.log2(math.e)
alpha = math.sqrt(unit)
kappa = unit * cut_square
tail = 2.0**-kappa
shift_big = 2.0 * kappa / (cut_square * density_rate)
density_scale = tail / kappa**2
energy_scale = 0.25 * tail**2 / kappa**2
force_scale = -2.0 * tail**2 * density_rate / (kappa**2 * alpha)
slope_scale = -0.5 / tail

AXES = ("gx", "gy", "gz")
DIRECTIONS = [
    (a, b, c)
    for a in (-1, 0, 1)
    for b in (-1, 0, 1)
    for c in (-1, 0, 1)
    if (a, b, c) != (0, 0, 0)
]


def kernel(dims, axis_sizes, pay_ref, out_ref, pad, pad_phi, spread, spread_phi, own, hot, block,
           pair_e, pair_m, pair_q, send_sem, recv_sem, send_phi, recv_phi):
    nx, ny, nz, slots = dims
    lanes = nz * slots
    me = [lax.axis_index(axis) for axis in AXES]

    def peer(direction):
        return {
            axis: lax.rem(place + step + size, size)
            for axis, place, step, size in zip(AXES, me, direction, axis_sizes)
        }

    barrier = pltpu.get_barrier_semaphore()
    for direction in DIRECTIONS:
        pl.semaphore_signal(
            barrier, inc=1, device_id=peer(direction), device_id_type=pl.DeviceIdType.MESH
        )
    pl.semaphore_wait(barrier, len(DIRECTIONS))

    def source_range(step, length):
        return pl.ds(length - 1, 1) if step > 0 else pl.ds(0, 1) if step < 0 else pl.ds(0, length)

    def target_range(step, length):
        return pl.ds(0, 1) if step > 0 else pl.ds(length + 1, 1) if step < 0 else pl.ds(1, length)

    copies = []
    for index, direction in enumerate(DIRECTIONS):
        a, b, c = direction
        zs = source_range(c, nz)
        copy = pltpu.make_async_remote_copy(
            src_ref=pay_ref.at[source_range(a, nx), source_range(b, ny), zs],
            dst_ref=pad.at[target_range(a, nx), target_range(b, ny), 1 - c, zs],
            send_sem=send_sem.at[index],
            recv_sem=recv_sem.at[index],
            device_id=peer(direction),
            device_id_type=pl.DeviceIdType.MESH,
        )
        copy.start()
        copies.append(copy)

    row = lax.broadcasted_iota(jnp.int32, (9 * nz, lanes), 0) % (3 * nz)
    cell = lax.broadcasted_iota(jnp.int32, (9 * nz, lanes), 1) // slots
    for dz in range(3):
        hot[:, dz * lanes : (dz + 1) * lanes] = jnp.where(
            row == cell + (nz - 1 + dz), 1.0, 0.0
        ).astype(jnp.bfloat16)
    block_row = lax.broadcasted_iota(jnp.int32, (lanes, lanes), 0) // slots
    block_col = lax.broadcasted_iota(jnp.int32, (lanes, lanes), 1) // slots
    block[...] = jnp.where(block_row == block_col, 1.0, 0.0).astype(jnp.bfloat16)
    diagonal = (
        lax.broadcasted_iota(jnp.int32, (slots, lanes), 1) % slots
        == lax.broadcasted_iota(jnp.int32, (slots, lanes), 0)
    )

    for x in range(nx):
        for y in range(ny):
            pad[x + 1, y + 1, 1] = pay_ref[x, y]

    for copy in copies:
        copy.wait()

    zrow = lax.broadcasted_iota(jnp.int32, (3 * nz, 4 * slots), 0)
    valid = (zrow >= nz - 1) & (zrow <= 2 * nz)

    def pieces(value):
        high = value.astype(jnp.bfloat16).astype(jnp.float32)
        rest = value - high
        middle = rest.astype(jnp.bfloat16).astype(jnp.float32)
        return high, middle, rest - middle

    def expand(t, carry):
        x, y = t // (ny + 2), t % (ny + 2)
        value = jnp.concatenate([pad[x, y, 0], pad[x, y, 1], pad[x, y, 2]], axis=0)
        value = jnp.where(valid, value, 0.0)
        stacked = jnp.concatenate(pieces(value), axis=0).astype(jnp.bfloat16)
        for dz in range(3):
            spread[x, y, dz] = lax.dot_general(
                stacked,
                hot[:, dz * lanes : (dz + 1) * lanes],
                (((0,), (0,)), ((), ())),
                preferred_element_type=jnp.float32,
            )
        return carry

    lax.fori_loop(0, (nx + 2) * (ny + 2), expand, 0)

    def density(t, carry):
        x, y = t // ny, t % ny
        mine = [
            jnp.sum(
                jnp.where(diagonal, spread[x + 1, y + 1, 1, k * slots : (k + 1) * slots, :], 0.0),
                axis=0,
                keepdims=True,
            )
            for k in range(4)
        ]
        for k in range(4):
            own[t, k : k + 1, :] = mine[k]

        def step(n, sums):
            rho, energy = sums
            a, b = n // 3, n % 3
            px = jnp.broadcast_to(mine[0] - (a - 1).astype(jnp.float32) * alpha, (8, lanes))
            py = jnp.broadcast_to(mine[1] - (b - 1).astype(jnp.float32) * alpha, (8, lanes))
            for dz in range(3):
                pz = jnp.broadcast_to(mine[2] - (dz - 1) * alpha, (8, lanes))
                for r in range(0, slots, 8):
                    dx = spread[x + a, y + b, dz, r : r + 8, :] - px
                    dy = spread[x + a, y + b, dz, slots + r : slots + r + 8, :] - py
                    dd = spread[x + a, y + b, dz, 2 * slots + r : 2 * slots + r + 8, :] - pz
                    wj = spread[x + a, y + b, dz, 3 * slots + r : 3 * slots + r + 8, :]
                    m = jnp.maximum(kappa - (dx * dx + dy * dy + dd * dd), 0.0)
                    e = jnp.exp2(m)
                    em = e * m
                    q = em * wj
                    rho = rho + q * m
                    energy = energy + q * em
                    pair_e[t, n, dz, r : r + 8, :] = e
                    pair_m[t, n, dz, r : r + 8, :] = m
                    pair_q[t, n, dz, r : r + 8, :] = q
            return rho, energy

        zero = jnp.zeros((8, lanes), jnp.float32)
        rho, energy = lax.fori_loop(0, 9, step, (zero, zero))
        w = mine[3]
        rho = jnp.sum(rho, axis=0, keepdims=True) * density_scale - w
        energy = jnp.sum(energy, axis=0, keepdims=True) * (energy_scale * w) - 0.25 * w * w
        root = jnp.sqrt(jnp.maximum(rho, 0.0) + 1.0)
        big = w > 1.3
        ratio = jnp.where(big, 0.875, jnp.where(w > 0.5, 1.0, 0.0))
        a = jnp.where(big, 1.4, jnp.where(w > 0.5, 1.0, 0.0))
        phi = slope_scale * ratio / root
        out_ref[t, 3:4, :] = energy - a * root
        pad_phi[x + 1, y + 1, :, 128 : 128 + lanes] = phi
        return carry

    lax.fori_loop(0, nx * ny, density, 0)

    def lane_source(step):
        return (
            pl.ds(lanes, 128) if step > 0 else pl.ds(128, 128) if step < 0 else pl.ds(128, lanes)
        )

    def lane_target(step):
        return (
            pl.ds(0, 128)
            if step > 0
            else pl.ds(128 + lanes, 128)
            if step < 0
            else pl.ds(128, lanes)
        )

    def inner_source(step, length):
        return pl.ds(length, 1) if step > 0 else pl.ds(1, 1) if step < 0 else pl.ds(1, length)

    copies = []
    for index, direction in enumerate(DIRECTIONS):
        a, b, c = direction
        copy = pltpu.make_async_remote_copy(
            src_ref=pad_phi.at[inner_source(a, nx), inner_source(b, ny), :, lane_source(c)],
            dst_ref=pad_phi.at[target_range(a, nx), target_range(b, ny), :, lane_target(c)],
            send_sem=send_phi.at[index],
            recv_sem=recv_phi.at[index],
            device_id=peer(direction),
            device_id_type=pl.DeviceIdType.MESH,
        )
        copy.start()
        copies.append(copy)
    for copy in copies:
        copy.wait()

    def expand_phi(t, carry):
        x, y = t // (ny + 2), t % (ny + 2)
        value = pad_phi[x, y]
        for dz in range(3):
            start = 128 + (dz - 1) * slots
            part = jnp.where(diagonal, value[:, start : start + lanes], 0.0)
            stacked = jnp.concatenate(pieces(part), axis=0).astype(jnp.bfloat16)
            result = jnp.dot(stacked, block[...], preferred_element_type=jnp.float32)
            spread_phi[x, y, dz] = (
                result[:slots] + result[slots : 2 * slots] + result[2 * slots :]
            )
        return carry

    lax.fori_loop(0, (nx + 2) * (ny + 2), expand_phi, 0)

    def force(t, carry):
        x, y = t // ny, t % ny
        mine = [own[t, k : k + 1, :] for k in range(4)]
        phi = jnp.broadcast_to(pad_phi[x + 1, y + 1, :, 128 : 128 + lanes], (8, lanes))

        def step(n, sums):
            fx, fy, fz = sums
            a, b = n // 3, n % 3
            px = jnp.broadcast_to(mine[0] - (a - 1).astype(jnp.float32) * alpha, (8, lanes))
            py = jnp.broadcast_to(mine[1] - (b - 1).astype(jnp.float32) * alpha, (8, lanes))
            for dz in range(3):
                pz = jnp.broadcast_to(mine[2] - (dz - 1) * alpha, (8, lanes))
                for r in range(0, slots, 8):
                    dx = spread[x + a, y + b, dz, r : r + 8, :] - px
                    dy = spread[x + a, y + b, dz, slots + r : slots + r + 8, :] - py
                    dd = spread[x + a, y + b, dz, 2 * slots + r : 2 * slots + r + 8, :] - pz
                    e = pair_e[t, n, dz, r : r + 8, :]
                    m = pair_m[t, n, dz, r : r + 8, :]
                    q = pair_q[t, n, dz, r : r + 8, :]
                    both = phi + spread_phi[x + a, y + b, dz, r : r + 8, :]
                    v = q * (both * (m + shift_big) + e * (m + 0.5 * shift_big))
                    fx = fx + v * dx
                    fy = fy + v * dy
                    fz = fz + v * dd
            return fx, fy, fz

        zero = jnp.zeros((8, lanes), jnp.float32)
        sums = lax.fori_loop(0, 9, step, (zero, zero, zero))
        scale = force_scale * mine[3]
        for k in range(3):
            out_ref[t, k : k + 1, :] = jnp.sum(sums[k], axis=0, keepdims=True) * scale
        return carry

    lax.fori_loop(0, nx * ny, force, 0)


def body(axis_sizes, positions, types):
    nx, ny, nz, slots = types.shape
    lanes = nz * slots
    weight = jnp.where(types == 1, 1.0, jnp.where(types == 2, 1.6, 0.0)).astype(jnp.float32)
    payload = jnp.concatenate([positions * alpha, weight], axis=3)
    count = len(DIRECTIONS)
    columns = nx * ny
    out = pl.pallas_call(
        functools.partial(kernel, (nx, ny, nz, slots), axis_sizes),
        out_shape=jax.ShapeDtypeStruct((columns, 4, lanes), jnp.float32),
        in_specs=[pl.BlockSpec(memory_space=pltpu.VMEM)],
        out_specs=pl.BlockSpec(memory_space=pltpu.VMEM),
        scratch_shapes=[
            pltpu.VMEM((nx + 2, ny + 2, 3, nz, 4 * slots), jnp.float32),
            pltpu.VMEM((nx + 2, ny + 2, 1, lanes + 256), jnp.float32),
            pltpu.VMEM((nx + 2, ny + 2, 3, 4 * slots, lanes), jnp.float32),
            pltpu.VMEM((nx + 2, ny + 2, 3, slots, lanes), jnp.float32),
            pltpu.VMEM((columns, 8, lanes), jnp.float32),
            pltpu.VMEM((9 * nz, 3 * lanes), jnp.bfloat16),
            pltpu.VMEM((lanes, lanes), jnp.bfloat16),
            pltpu.VMEM((columns, 9, 3, slots, lanes), jnp.float32),
            pltpu.VMEM((columns, 9, 3, slots, lanes), jnp.float32),
            pltpu.VMEM((columns, 9, 3, slots, lanes), jnp.float32),
            pltpu.SemaphoreType.DMA((count,)),
            pltpu.SemaphoreType.DMA((count,)),
            pltpu.SemaphoreType.DMA((count,)),
            pltpu.SemaphoreType.DMA((count,)),
        ],
        compiler_params=pltpu.CompilerParams(
            collective_id=0, has_side_effects=True, vmem_limit_bytes=60 * 1024 * 1024
        ),
    )(payload)
    out = out.reshape(nx, ny, 4, nz, slots).transpose(0, 1, 3, 2, 4)
    return out.reshape(nx, ny, nz, 4 * slots)


def solution(mesh):
    spec = P("gx", "gy", "gz", None)
    sizes = tuple(mesh.shape[axis] for axis in AXES)
    return jax.shard_map(
        functools.partial(body, sizes),
        mesh=mesh,
        in_specs=(spec, spec),
        out_specs=spec,
        check_vma=False,
    )
```

```python
import functools
import math

import jax
import jax.numpy as jnp
from jax import lax
from jax.experimental import pallas as pl
from jax.experimental.pallas import tpu as pltpu
from jax.sharding import PartitionSpec as P

cut_square = 0.9025
density_rate = 3.0
unit = density_rate * math.log2(math.e)
alpha = math.sqrt(unit)
kappa = unit * cut_square
tail = 2.0**-kappa
shift_big = 2.0 * kappa / (cut_square * density_rate)
density_scale = tail / kappa**2
energy_scale = 0.25 * tail**2 / kappa**2
force_scale = -2.0 * tail**2 * density_rate / (kappa**2 * alpha)
slope_scale = -0.5 / tail

AXES = ("gx", "gy", "gz")
DIRECTIONS = [
    (a, b, c)
    for a in (-1, 0, 1)
    for b in (-1, 0, 1)
    for c in (-1, 0, 1)
    if (c != 0) != ((a, b) != (0, 0))
]


def kernel(dims, axis_sizes, pay_ref, out_ref, pad, pad_phi, spread, spread_phi, own, hot, block,
           pair_e, pair_m, pair_q, send_sem, recv_sem, send_phi, recv_phi):
    nx, ny, nz, slots = dims
    lanes = nz * slots
    me = [lax.axis_index(axis) for axis in AXES]

    def peer(direction):
        return {
            axis: lax.rem(place + step + size, size)
            for axis, place, step, size in zip(AXES, me, direction, axis_sizes)
        }

    barrier = pltpu.get_barrier_semaphore()
    for direction in DIRECTIONS:
        pl.semaphore_signal(
            barrier, inc=1, device_id=peer(direction), device_id_type=pl.DeviceIdType.MESH
        )
    pl.semaphore_wait(barrier, len(DIRECTIONS))

    def source_range(step, length):
        return pl.ds(length - 1, 1) if step > 0 else pl.ds(0, 1) if step < 0 else pl.ds(0, length)

    def target_range(step, length):
        return pl.ds(0, 1) if step > 0 else pl.ds(length + 1, 1) if step < 0 else pl.ds(1, length)

    def column_source(step, length):
        return pl.ds(length, 1) if step > 0 else pl.ds(1, 1) if step < 0 else pl.ds(1, length)

    def send(index, source, target, send_sems, recv_sems):
        copy = pltpu.make_async_remote_copy(
            src_ref=source,
            dst_ref=target,
            send_sem=send_sems.at[index],
            recv_sem=recv_sems.at[index],
            device_id=peer(DIRECTIONS[index]),
            device_id_type=pl.DeviceIdType.MESH,
        )
        copy.start()
        return copy

    along = [k for k, d in enumerate(DIRECTIONS) if d[2] != 0]
    across = [k for k, d in enumerate(DIRECTIONS) if d[2] == 0]

    def send_across(array, send_sems, recv_sems):
        copies = []
        for k in across:
            a, b, _ = DIRECTIONS[k]
            copies.append(
                send(
                    k,
                    array.at[column_source(a, nx), column_source(b, ny)],
                    array.at[target_range(a, nx), target_range(b, ny)],
                    send_sems,
                    recv_sems,
                )
            )
        return copies

    copies = []
    for k in along:
        c = DIRECTIONS[k][2]
        zs = source_range(c, nz)
        copies.append(
            send(
                k,
                pay_ref.at[:, :, zs],
                pad.at[pl.ds(1, nx), pl.ds(1, ny), 1 - c, zs],
                send_sem,
                recv_sem,
            )
        )
    for x in range(nx):
        for y in range(ny):
            pad[x + 1, y + 1, 1] = pay_ref[x, y]
    for copy in copies:
        copy.wait()
    copies = send_across(pad, send_sem, recv_sem)

    row = lax.broadcasted_iota(jnp.int32, (9 * nz, lanes), 0) % (3 * nz)
    cell = lax.broadcasted_iota(jnp.int32, (9 * nz, lanes), 1) // slots
    for dz in range(3):
        hot[:, dz * lanes : (dz + 1) * lanes] = jnp.where(
            row == cell + (nz - 1 + dz), 1.0, 0.0
        ).astype(jnp.bfloat16)
    block_row = lax.broadcasted_iota(jnp.int32, (lanes, lanes), 0) // slots
    block_col = lax.broadcasted_iota(jnp.int32, (lanes, lanes), 1) // slots
    block[...] = jnp.where(block_row == block_col, 1.0, 0.0).astype(jnp.bfloat16)
    diagonal = (
        lax.broadcasted_iota(jnp.int32, (slots, lanes), 1) % slots
        == lax.broadcasted_iota(jnp.int32, (slots, lanes), 0)
    )

    for copy in copies:
        copy.wait()

    zrow = lax.broadcasted_iota(jnp.int32, (3 * nz, 4 * slots), 0)
    valid = (zrow >= nz - 1) & (zrow <= 2 * nz)

    def pieces(value):
        high = value.astype(jnp.bfloat16).astype(jnp.float32)
        rest = value - high
        middle = rest.astype(jnp.bfloat16).astype(jnp.float32)
        return high, middle, rest - middle

    def expand(t, carry):
        x, y = t // (ny + 2), t % (ny + 2)
        value = jnp.concatenate([pad[x, y, 0], pad[x, y, 1], pad[x, y, 2]], axis=0)
        value = jnp.where(valid, value, 0.0)
        stacked = jnp.concatenate(pieces(value), axis=0).astype(jnp.bfloat16)
        for dz in range(3):
            spread[x, y, dz] = lax.dot_general(
                stacked,
                hot[:, dz * lanes : (dz + 1) * lanes],
                (((0,), (0,)), ((), ())),
                preferred_element_type=jnp.float32,
            )
        return carry

    lax.fori_loop(0, (nx + 2) * (ny + 2), expand, 0)

    def density(t, carry):
        x, y = t // ny, t % ny
        mine = [
            jnp.sum(
                jnp.where(diagonal, spread[x + 1, y + 1, 1, k * slots : (k + 1) * slots, :], 0.0),
                axis=0,
                keepdims=True,
            )
            for k in range(4)
        ]
        for k in range(4):
            own[t, k : k + 1, :] = mine[k]

        def step(n, sums):
            rho, energy = sums
            a, b = n // 3, n % 3
            px = jnp.broadcast_to(mine[0] - (a - 1).astype(jnp.float32) * alpha, (8, lanes))
            py = jnp.broadcast_to(mine[1] - (b - 1).astype(jnp.float32) * alpha, (8, lanes))
            for dz in range(3):
                pz = jnp.broadcast_to(mine[2] - (dz - 1) * alpha, (8, lanes))
                for r in range(0, slots, 8):
                    dx = spread[x + a, y + b, dz, r : r + 8, :] - px
                    dy = spread[x + a, y + b, dz, slots + r : slots + r + 8, :] - py
                    dd = spread[x + a, y + b, dz, 2 * slots + r : 2 * slots + r + 8, :] - pz
                    wj = spread[x + a, y + b, dz, 3 * slots + r : 3 * slots + r + 8, :]
                    m = jnp.maximum(kappa - (dx * dx + dy * dy + dd * dd), 0.0)
                    e = jnp.exp2(m)
                    em = e * m
                    q = em * wj
                    rho = rho + q * m
                    energy = energy + q * em
                    pair_e[t, n, dz, r : r + 8, :] = e
                    pair_m[t, n, dz, r : r + 8, :] = m
                    pair_q[t, n, dz, r : r + 8, :] = q
            return rho, energy

        zero = jnp.zeros((8, lanes), jnp.float32)
        rho, energy = lax.fori_loop(0, 9, step, (zero, zero))
        w = mine[3]
        rho = jnp.sum(rho, axis=0, keepdims=True) * density_scale - w
        energy = jnp.sum(energy, axis=0, keepdims=True) * (energy_scale * w) - 0.25 * w * w
        root = jnp.sqrt(jnp.maximum(rho, 0.0) + 1.0)
        big = w > 1.3
        ratio = jnp.where(big, 0.875, jnp.where(w > 0.5, 1.0, 0.0))
        a = jnp.where(big, 1.4, jnp.where(w > 0.5, 1.0, 0.0))
        phi = slope_scale * ratio / root
        out_ref[t, 3:4, :] = energy - a * root
        pad_phi[x + 1, y + 1, :, 128 : 128 + lanes] = phi
        return carry

    lax.fori_loop(0, nx * ny, density, 0)

    def lane_source(step):
        return (
            pl.ds(lanes, 128) if step > 0 else pl.ds(128, 128) if step < 0 else pl.ds(128, lanes)
        )

    def lane_target(step):
        return (
            pl.ds(0, 128)
            if step > 0
            else pl.ds(128 + lanes, 128)
            if step < 0
            else pl.ds(128, lanes)
        )

    copies = []
    for k in along:
        c = DIRECTIONS[k][2]
        copies.append(
            send(
                k,
                pad_phi.at[pl.ds(1, nx), pl.ds(1, ny), :, lane_source(c)],
                pad_phi.at[pl.ds(1, nx), pl.ds(1, ny), :, lane_target(c)],
                send_phi,
                recv_phi,
            )
        )
    for copy in copies:
        copy.wait()
    for copy in send_across(pad_phi, send_phi, recv_phi):
        copy.wait()

    def expand_phi(t, carry):
        x, y = t // (ny + 2), t % (ny + 2)
        value = pad_phi[x, y]
        for dz in range(3):
            start = 128 + (dz - 1) * slots
            part = jnp.where(diagonal, value[:, start : start + lanes], 0.0)
            stacked = jnp.concatenate(pieces(part), axis=0).astype(jnp.bfloat16)
            result = jnp.dot(stacked, block[...], preferred_element_type=jnp.float32)
            spread_phi[x, y, dz] = (
                result[:slots] + result[slots : 2 * slots] + result[2 * slots :]
            )
        return carry

    lax.fori_loop(0, (nx + 2) * (ny + 2), expand_phi, 0)

    def force(t, carry):
        x, y = t // ny, t % ny
        mine = [own[t, k : k + 1, :] for k in range(4)]
        phi = jnp.broadcast_to(pad_phi[x + 1, y + 1, :, 128 : 128 + lanes], (8, lanes))

        def step(n, sums):
            fx, fy, fz = sums
            a, b = n // 3, n % 3
            px = jnp.broadcast_to(mine[0] - (a - 1).astype(jnp.float32) * alpha, (8, lanes))
            py = jnp.broadcast_to(mine[1] - (b - 1).astype(jnp.float32) * alpha, (8, lanes))
            for dz in range(3):
                pz = jnp.broadcast_to(mine[2] - (dz - 1) * alpha, (8, lanes))
                for r in range(0, slots, 8):
                    dx = spread[x + a, y + b, dz, r : r + 8, :] - px
                    dy = spread[x + a, y + b, dz, slots + r : slots + r + 8, :] - py
                    dd = spread[x + a, y + b, dz, 2 * slots + r : 2 * slots + r + 8, :] - pz
                    e = pair_e[t, n, dz, r : r + 8, :]
                    m = pair_m[t, n, dz, r : r + 8, :]
                    q = pair_q[t, n, dz, r : r + 8, :]
                    both = phi + spread_phi[x + a, y + b, dz, r : r + 8, :]
                    v = q * (both * (m + shift_big) + e * (m + 0.5 * shift_big))
                    fx = fx + v * dx
                    fy = fy + v * dy
                    fz = fz + v * dd
            return fx, fy, fz

        zero = jnp.zeros((8, lanes), jnp.float32)
        sums = lax.fori_loop(0, 9, step, (zero, zero, zero))
        scale = force_scale * mine[3]
        for k in range(3):
            out_ref[t, k : k + 1, :] = jnp.sum(sums[k], axis=0, keepdims=True) * scale
        return carry

    lax.fori_loop(0, nx * ny, force, 0)


def body(axis_sizes, positions, types):
    nx, ny, nz, slots = types.shape
    lanes = nz * slots
    weight = jnp.where(types == 1, 1.0, jnp.where(types == 2, 1.6, 0.0)).astype(jnp.float32)
    payload = jnp.concatenate([positions * alpha, weight], axis=3)
    count = len(DIRECTIONS)
    columns = nx * ny
    out = pl.pallas_call(
        functools.partial(kernel, (nx, ny, nz, slots), axis_sizes),
        out_shape=jax.ShapeDtypeStruct((columns, 4, lanes), jnp.float32),
        in_specs=[pl.BlockSpec(memory_space=pltpu.VMEM)],
        out_specs=pl.BlockSpec(memory_space=pltpu.VMEM),
        scratch_shapes=[
            pltpu.VMEM((nx + 2, ny + 2, 3, nz, 4 * slots), jnp.float32),
            pltpu.VMEM((nx + 2, ny + 2, 1, lanes + 256), jnp.float32),
            pltpu.VMEM((nx + 2, ny + 2, 3, 4 * slots, lanes), jnp.float32),
            pltpu.VMEM((nx + 2, ny + 2, 3, slots, lanes), jnp.float32),
            pltpu.VMEM((columns, 8, lanes), jnp.float32),
            pltpu.VMEM((9 * nz, 3 * lanes), jnp.bfloat16),
            pltpu.VMEM((lanes, lanes), jnp.bfloat16),
            pltpu.VMEM((columns, 9, 3, slots, lanes), jnp.float32),
            pltpu.VMEM((columns, 9, 3, slots, lanes), jnp.float32),
            pltpu.VMEM((columns, 9, 3, slots, lanes), jnp.float32),
            pltpu.SemaphoreType.DMA((count,)),
            pltpu.SemaphoreType.DMA((count,)),
            pltpu.SemaphoreType.DMA((count,)),
            pltpu.SemaphoreType.DMA((count,)),
        ],
        compiler_params=pltpu.CompilerParams(
            collective_id=0, has_side_effects=True, vmem_limit_bytes=60 * 1024 * 1024
        ),
    )(payload)
    out = out.reshape(nx, ny, 4, nz, slots).transpose(0, 1, 3, 2, 4)
    return out.reshape(nx, ny, nz, 4 * slots)


def solution(mesh):
    spec = P("gx", "gy", "gz", None)
    sizes = tuple(mesh.shape[axis] for axis in AXES)
    return jax.shard_map(
        functools.partial(body, sizes),
        mesh=mesh,
        in_specs=(spec, spec),
        out_specs=spec,
        check_vma=False,
    )
```
